32 devices in a mesh: kpt: 2 (over x), col: 4 (over z), row: 4 (over y, core).
Axes of the slice: x: 2, y: 2, z: 4, core: 2. Of those that a mesh axis runs over, the one named last changes fastest.
Arguments:
- h_slab: bfloat16 [8, 4, 2560, 5120], P(('kpt', 'row'), 'col'), parts along dimension 0
- h_diag: bfloat16 [8, 5120, 5120], P(('kpt', 'row'), 'col'), parts along dimension 0
- vec_occ: float32 [40960, 64], P(('kpt', 'row', 'col')), parts along dimension 0
- vec_virt: float32 [40960, 64], P(('kpt', 'row', 'col')), parts along dimension 0
Outputs:
- output 1: float32 [40960, 64], P(('kpt', 'row', 'col')), parts along dimension 0
- output 2: float32 [40960, 64], P(('kpt', 'row', 'col')), parts along dimension 0
There are 2 independent parts. The reference program is written for one: setup_inputs(seed, part) draws one part's arguments, and reference() takes and returns one part's arrays. A program takes and returns all parts, laid end to end along the dimension named above; each array names one.
All inputs are finite; a program needn't handle non-finite values.
Results may differ from the reference program's by a relative error of at most 0.001.
Values are sent between devices in bfloat16 or wider.
A program may use at most 1 GiB of HBM per device.

```python
import jax
import jax.numpy as jnp
from jax import lax

GRID_SIDE = 4
MAT_ORDER = 20480
NUM_VECS = 128
FILTER_STEPS = 3
BLOCK_ROWS = MAT_ORDER // GRID_SIDE
HALF_ROWS = BLOCK_ROWS // 2
HALF_VECS = NUM_VECS // 2
CEN_OCC = 0.5
HW_OCC = 1.5
CEN_VIRT = -0.5
HW_VIRT = 1.5


def setup_inputs(seed: int = 0, part: int = 0) -> dict:
    base_key = jax.random.fold_in(jax.random.key(seed), part)
    k_slab, k_diag, k_occ, k_virt = jax.random.split(base_key, 4)
    entry_scale = MAT_ORDER ** -0.5
    h_slab = jax.random.normal(k_slab, (GRID_SIDE, GRID_SIDE, HALF_ROWS, BLOCK_ROWS), jnp.float32) * entry_scale
    gauss_draw = jax.random.normal(k_diag, (GRID_SIDE, BLOCK_ROWS, BLOCK_ROWS), jnp.float32)
    h_diag = (gauss_draw + jnp.swapaxes(gauss_draw, 1, 2)) * (entry_scale * 0.5 ** 0.5)
    vec_occ = jax.random.normal(k_occ, (MAT_ORDER, HALF_VECS), jnp.float32)
    vec_virt = jax.random.normal(k_virt, (MAT_ORDER, HALF_VECS), jnp.float32)
    return {"h_slab": h_slab.astype(jnp.bfloat16), "h_diag": h_diag.astype(jnp.bfloat16), "vec_occ": vec_occ, "vec_virt": vec_virt}


def apply_op(h_slab, h_diag, panel):
    grid_ids = jnp.arange(GRID_SIDE)

    def row_step(row_acc, scan_in):
        row_id, slab_row = scan_in
        slab_row = slab_row.astype(jnp.float32)
        low_slab = slab_row * (grid_ids < row_id).astype(jnp.float32)[:, None, None]
        up_slab = slab_row * (grid_ids > row_id).astype(jnp.float32)[:, None, None]
        own_panel = panel[row_id]
        top_part = jnp.einsum("cij,cjk->ik", low_slab, panel)
        side_part = jnp.einsum("cij,cik->jk", up_slab, panel[:, HALF_ROWS:])
        own_rows = side_part + jnp.concatenate([top_part, jnp.zeros_like(top_part)], axis=0)
        bottom_part = jnp.einsum("cij,jk->cik", up_slab, own_panel)
        tran_part = jnp.einsum("cij,ik->cjk", low_slab, own_panel[:HALF_ROWS])
        row_acc = row_acc + tran_part + jnp.concatenate([jnp.zeros_like(bottom_part), bottom_part], axis=1)
        return row_acc, own_rows

    row_acc, own_rows = lax.scan(row_step, jnp.zeros_like(panel), (grid_ids, h_slab))
    diag_part = jnp.einsum("aij,ajk->aik", h_diag.astype(jnp.float32), panel)
    return row_acc + own_rows + diag_part


def reference(h_slab, h_diag, vec_occ, vec_virt):
    col_shift = jnp.concatenate([jnp.full((HALF_VECS,), CEN_OCC, jnp.float32), jnp.full((HALF_VECS,), CEN_VIRT, jnp.float32)])
    col_scale = jnp.concatenate([jnp.full((HALF_VECS,), 1.0 / HW_OCC, jnp.float32), jnp.full((HALF_VECS,), 1.0 / HW_VIRT, jnp.float32)])

    def filter_op(cur_vecs):
        wire_vecs = cur_vecs.astype(jnp.bfloat16).astype(jnp.float32)
        return (apply_op(h_slab, h_diag, wire_vecs) - col_shift * cur_vecs) * col_scale

    prev_vecs = jnp.concatenate([vec_occ, vec_virt], axis=1).reshape(GRID_SIDE, BLOCK_ROWS, NUM_VECS)
    cur_vecs = filter_op(prev_vecs)
    for _ in range(FILTER_STEPS - 1):
        next_vecs = 2.0 * filter_op(cur_vecs) - prev_vecs
        prev_vecs, cur_vecs = cur_vecs, next_vecs
    result_vecs = cur_vecs.reshape(MAT_ORDER, NUM_VECS)
    return result_vecs[:, :HALF_VECS], result_vecs[:, HALF_VECS:]
```

```python
import jax
import jax.numpy as jnp
from jax import lax
from jax.experimental import pallas as pl
from jax.experimental.pallas import tpu as pltpu
from jax.sharding import PartitionSpec as P

FILTER_STEPS = 3
CEN_OCC = 0.5
CEN_VIRT = -0.5
HALF_WIDTH = 1.5
SIDE = 4
HALVES = 2
UNITS = FILTER_STEPS * HALVES
DIAG_ACC = 8
MESH = pl.DeviceIdType.MESH
NN = (((1,), (0,)), ((), ()))
NT = (((1,), (1,)), ((), ()))


def filter_kernel(slab_hbm, strip_hbm, occ_ref, virt_ref, out_occ, out_virt,
                  mat, vec, acc, red, col, cur, prev,
                  mat_sem, vec_send, vec_recv, colvec_recv, acc_send, red_recv, col_recv):
    seg_rows = cur.shape[-1]
    kpt = lax.axis_index("kpt")
    c = lax.axis_index("col")
    r = lax.axis_index("row")
    is_diag = r == c
    lower = r > c
    upper = r < c
    chip = r // 2
    core = r % 2
    partner = r + 1 - 2 * core
    same_chip = (c // 2) == chip
    far0 = 2 * (1 - chip)
    col_peers = (partner, far0, far0 + 1)
    diag_dev = (kpt, c, c)

    def seg_order(i):
        ahead = jnp.where(c == 1, jnp.where(i < 2, 3 - i, i - 2), jnp.where(i < 2, i, 5 - i))
        return jnp.where(c == 0, 3 - i, jnp.where(c == 3, i, ahead))

    def goes_right(cc, seg):
        return (seg < 2) | (r <= cc)

    def goes_left(cc, seg):
        return ~((r == 3) & (cc == 3) & (seg < 2))

    def sends(seg):
        return jnp.where(seg > c, goes_right(c, seg), goes_left(c, seg)) & (seg != c)

    def from_left(seg):
        return (c > 0) & goes_right(c - 1, seg)

    def from_right(seg):
        return (c < 3) & goes_left(c + 1, seg)

    def incoming(seg):
        return jnp.where(seg > c, from_left(seg), from_right(seg))

    def row_copy(h, b, seg, way):
        return pltpu.make_async_remote_copy(
            src_ref=vec.at[h, b, 0, seg], dst_ref=vec.at[h, b, 0, seg],
            send_sem=vec_send.at[h, way, seg], recv_sem=vec_recv.at[h, b, seg],
            device_id=(kpt, c + 1 - 2 * way, r), device_id_type=MESH)

    def col_copy(h, b, seg, peer):
        return pltpu.make_async_remote_copy(
            src_ref=vec.at[h, b, 0, seg], dst_ref=vec.at[h, b, 1, seg],
            send_sem=vec_send.at[h, 2 + peer, seg], recv_sem=colvec_recv.at[h, b, seg],
            device_id=(kpt, c, col_peers[peer]), device_id_type=MESH)

    def red_copy(h, seg):
        step = jnp.where(seg > c, 1, -1)
        slot = jnp.where(seg == c - 1, SIDE, seg)
        return pltpu.make_async_remote_copy(
            src_ref=acc.at[h, seg], dst_ref=red.at[h, slot],
            send_sem=acc_send.at[h, seg], recv_sem=red_recv.at[h, slot],
            device_id=(kpt, c + step, r), device_id_type=MESH)

    def sum_copy(h, seg, slot, dev):
        return pltpu.make_async_remote_copy(
            src_ref=acc.at[h, SIDE + seg], dst_ref=col.at[h, slot, seg],
            send_sem=acc_send.at[h, SIDE + seg], recv_sem=col_recv.at[h, slot, seg],
            device_id=dev, device_id_type=MESH)

    def send_row(h, b, seg, left_ok, right_ok):
        @pl.when((c < 3) & right_ok)
        def _():
            row_copy(h, b, seg, 0).start()

        @pl.when((c > 0) & left_ok)
        def _():
            row_copy(h, b, seg, 1).start()

    def send_col(h, b, seg):
        for peer in range(3):
            @pl.when(is_diag & ((col_peers[peer] > c) | (seg >= 2)))
            def _():
                col_copy(h, b, seg, peer).start()

    def wait_vec_sends(h, b):
        def each(seg, carry):
            @pl.when((c < 3) & (seg <= c))
            def _():
                row_copy(h, b, seg, 0).wait_send()

            @pl.when((c > 0) & (seg >= c))
            def _():
                row_copy(h, b, seg, 1).wait_send()

            for peer in range(3):
                @pl.when(is_diag & ((col_peers[peer] > c) | (seg >= 2)))
                def _():
                    col_copy(h, b, seg, peer).wait_send()
            return carry

        lax.fori_loop(0, SIDE, each, 0)

    def wait_acc_sends(h):
        def each(seg, carry):
            @pl.when(sends(seg))
            def _():
                red_copy(h, seg).wait_send()

            @pl.when(~is_diag & (lower | (seg >= 2)))
            def _():
                sum_copy(h, seg, 0, diag_dev).wait_send()
            return carry

        lax.fori_loop(0, SIDE, each, 0)

    def wait_colvec(h, b, seg):
        col_copy(h, b, seg, 0).wait_recv()

    def send_sum(h, seg):
        @pl.when(same_chip)
        def _():
            sum_copy(h, seg, 0, diag_dev).start()

        @pl.when(~same_chip & (seg % 2 != core))
        def _():
            sum_copy(h, seg, 0, (kpt, c, partner)).start()

    def combine_sums(h):
        first = jnp.where(lower, 0, 1)

        def each(i, carry):
            seg = 2 * i + core
            sum_copy(h, seg, 0, diag_dev).wait_recv()
            acc[h, SIDE + seg] += col[h, 0, seg]
            sum_copy(h, seg, 1, diag_dev).start()
            return carry

        @pl.when(~same_chip)
        def _():
            lax.fori_loop(first, 2, each, 0)

    def column_total(h):
        def each(i, carry):
            seg = seg_order(i)
            near = (partner > c) | (seg >= 2)
            far = (far0 > c) | (seg >= 2)

            @pl.when(near)
            def _():
                sum_copy(h, seg, 0, diag_dev).wait_recv()
                acc[h, seg] += col[h, 0, seg]

            @pl.when(far)
            def _():
                sum_copy(h, seg, 1, diag_dev).wait_recv()
                acc[h, seg] += col[h, 1, seg]

            @pl.when(sends(seg) & ~incoming(seg))
            def _():
                red_copy(h, seg).start()
            return carry

        lax.fori_loop(0, SIDE, each, 0)

    def relay(h, seg):
        @pl.when(sends(seg) & incoming(seg))
        def _():
            pltpu.make_async_remote_copy(
                src_ref=acc.at[h, seg], dst_ref=red.at[h, seg],
                send_sem=acc_send.at[h, seg], recv_sem=red_recv.at[h, seg],
                device_id=diag_dev, device_id_type=MESH).wait_recv()
            acc[h, seg] += red[h, seg]
            red_copy(h, seg).start()

    def take_piece(k, h, b, seg):
        n_nt = jnp.where(upper, 3, 1)
        n_nn = jnp.where(lower & (seg < 2), SIDE, 0)

        def nt_step(i, carry):
            block = jnp.where(i == 0, 2 * SIDE + seg, (i - 1) * SIDE + seg)
            dest = jnp.where(i == 0, DIAG_ACC, SIDE + 1 + i)

            @pl.when(k == 0)
            def _():
                pltpu.make_async_copy(mat.at[block], mat.at[block], mat_sem.at[block]).wait()
            acc[h, dest] += lax.dot_general(vec[h, b, 0, seg], mat[block], NT, preferred_element_type=jnp.float32)
            return carry

        lax.fori_loop(0, n_nt, nt_step, 0)

        def nn_step(i, carry):
            block = seg * SIDE + i

            @pl.when(k == 0)
            def _():
                pltpu.make_async_copy(mat.at[block], mat.at[block], mat_sem.at[block]).wait()
            acc[h, SIDE + i] += lax.dot_general(vec[h, b, 0, seg], mat[block], NN, preferred_element_type=jnp.float32)
            return carry

        lax.fori_loop(0, n_nn, nn_step, 0)

    def upper_row_terms(h, b):
        def each(i, carry):
            seg = seg_order(i // 2)
            half = i % 2
            acc[h, seg] += lax.dot_general(
                vec[h, b, 1, 2 + half], mat[half * SIDE + seg], NN, preferred_element_type=jnp.float32)
            return carry

        lax.fori_loop(0, 2 * SIDE, each, 0)

    def lower_row_terms(h, b):
        def each(i, carry):
            seg = (i // 2 + c) % SIDE
            half = i % 2

            @pl.when((half == 0) & (i > 0))
            def _():
                wait_colvec(h, b, seg)
            acc[h, half] += lax.dot_general(
                vec[h, b, 1, seg], mat[half * SIDE + seg], NT, preferred_element_type=jnp.float32)
            return carry

        lax.fori_loop(0, 2 * SIDE, each, 0)

    def finish(k, h, b, next_b):
        wait_vec_sends(h, b)

        @pl.when(from_left(c))
        def _():
            pltpu.make_async_remote_copy(
                src_ref=acc.at[h, c], dst_ref=red.at[h, c],
                send_sem=acc_send.at[h, c], recv_sem=red_recv.at[h, c],
                device_id=diag_dev, device_id_type=MESH).wait_recv()
            acc[h, c] += red[h, c]

        @pl.when(from_right(c))
        def _():
            pltpu.make_async_remote_copy(
                src_ref=acc.at[h, c], dst_ref=red.at[h, SIDE],
                send_sem=acc_send.at[h, c], recv_sem=red_recv.at[h, SIDE],
                device_id=diag_dev, device_id_type=MESH).wait_recv()
            acc[h, c] += red[h, SIDE]

        center = jnp.where(h == 0, CEN_OCC, CEN_VIRT)
        applied = acc[h, c] + acc[h, DIAG_ACC]
        scaled = (applied - center * cur[h]) * (1.0 / HALF_WIDTH)
        first = k < HALVES
        nxt = jnp.where(first, scaled, 2.0 * scaled - prev[h])
        prev[h] = cur[h]
        cur[h] = nxt

        @pl.when(k + HALVES < UNITS)
        def _():
            vec[h, next_b, 0, c] = nxt.astype(jnp.bfloat16)
            send_row(h, next_b, c, True, True)
            send_col(h, next_b, c)

    barrier = pltpu.get_barrier_semaphore()

    @pl.when(c > 0)
    def _():
        pl.semaphore_signal(barrier, inc=1, device_id=(kpt, c - 1, r), device_id_type=MESH)

    @pl.when(c < 3)
    def _():
        pl.semaphore_signal(barrier, inc=1, device_id=(kpt, c + 1, r), device_id_type=MESH)

    for peer in range(3):
        pl.semaphore_signal(barrier, inc=1, device_id=(kpt, c, col_peers[peer]), device_id_type=MESH)

    def load_block(i, carry):
        seg = (c + i) % SIDE
        pltpu.make_async_copy(
            strip_hbm.at[:, pl.ds(pl.multiple_of(seg * seg_rows, seg_rows), seg_rows)],
            mat.at[2 * SIDE + seg], mat_sem.at[2 * SIDE + seg]).start()

        @pl.when(~is_diag)
        def _():
            for half in range(2):
                pltpu.make_async_copy(
                    slab_hbm.at[pl.ds(half * seg_rows, seg_rows),
                                pl.ds(pl.multiple_of(seg * seg_rows, seg_rows), seg_rows)],
                    mat.at[half * SIDE + seg], mat_sem.at[half * SIDE + seg]).start()
        return carry

    lax.fori_loop(0, SIDE, load_block, 0)
    for h, src in enumerate((occ_ref, virt_ref)):
        cur[h] = src[...]
        prev[h] = jnp.zeros_like(src)
        vec[h, 0, 0, c] = src[...].astype(jnp.bfloat16)
    pl.semaphore_wait(barrier, 3 + (c > 0).astype(jnp.int32) + (c < 3).astype(jnp.int32))
    for h in range(HALVES):
        send_row(h, 0, c, True, True)
        send_col(h, 0, c)

    def slot(k, carry):
        h = k % 2
        b = (k // 2) % 2
        last = k - 1
        lh = (k + 1) % 2
        lb = ((k + 1) // 2 + 1) % 2
        live = k < UNITS
        older = k >= 1

        @pl.when(live)
        def _():
            @pl.when(k >= HALVES)
            def _():
                wait_acc_sends(h)

            def clear(i, cc):
                acc[h, i] = jnp.zeros(acc.shape[2:], acc.dtype)
                return cc

            lax.fori_loop(0, DIAG_ACC + 1, clear, 0)

        def arrivals(d, cc):
            def side(s, ccc):
                seg = c + (2 * s - 1) * d
                valid = live & (seg >= 0) & (seg < SIDE) & ((d > 0) | (s == 0))

                @pl.when(valid)
                def _():
                    @pl.when(d > 0)
                    def _():
                        row_copy(h, b, seg, 0).wait_recv()
                        send_row(h, b, seg, s == 1, s == 0)
                        send_col(h, b, seg)
                    take_piece(k, h, b, seg)
                return ccc

            lax.fori_loop(0, 2, side, 0)

            @pl.when(live & lower & (d == jnp.where(c == 2, 2, 1)))
            def _():
                wait_colvec(h, b, c)

                def each(i, ccc):
                    send_sum(h, seg_order(i))
                    return ccc

                lax.fori_loop(0, SIDE, each, 0)

            @pl.when(live & lower & (d == 2))
            def _():
                combine_sums(h)

            @pl.when(older & is_diag & (c >= 2) & (d == 1))
            def _():
                column_total(lh)

            @pl.when(older & (c > 0) & (c < 3) & (d > 0))
            def _():
                relay(lh, jnp.where(c == 1, jnp.where(d == 3, 0, 4 - d), jnp.where(d == 3, 3, d - 1)))
            return cc

        lax.fori_loop(0, SIDE, arrivals, 0)

        @pl.when(live & upper)
        def _():
            wait_colvec(h, b, 2)
            wait_colvec(h, b, 3)
            send_sum(h, 2)
            send_sum(h, 3)
            upper_row_terms(h, b)
            combine_sums(h)

        @pl.when(live & lower)
        def _():
            lower_row_terms(h, b)

        @pl.when(older)
        def _():
            finish(last, lh, lb, 1 - lb)

        @pl.when(live & ~is_diag)
        def _():
            def each(i, cc):
                seg = seg_order(i)

                @pl.when(sends(seg) & ~incoming(seg))
                def _():
                    red_copy(h, seg).start()
                return cc

            lax.fori_loop(0, SIDE, each, 0)

        @pl.when(live & is_diag & (c < 2))
        def _():
            column_total(h)
        return carry

    lax.fori_loop(0, UNITS + 1, slot, 0)
    for h in range(HALVES):
        wait_acc_sends(h)
    out_occ[...] = cur[0]
    out_virt[...] = cur[1]


def solution(mesh):
    slab_spec = P(("kpt", "row"), "col", None, None)
    diag_spec = P(("kpt", "row"), "col", None)
    vec_spec = P(("kpt", "row", "col"), None)

    def local_filter(h_slab, h_diag, vec_occ, vec_virt):
        seg_rows, n_vecs = vec_occ.shape
        panel = (n_vecs, seg_rows)
        out = jax.ShapeDtypeStruct(panel, jnp.float32)
        vmem = pl.BlockSpec(memory_space=pltpu.VMEM)
        hbm = pl.BlockSpec(memory_space=pl.ANY)
        dma = pltpu.SemaphoreType.DMA
        filt_occ, filt_virt = pl.pallas_call(
            filter_kernel,
            out_shape=(out, out),
            in_specs=[hbm, hbm, vmem, vmem],
            out_specs=(vmem, vmem),
            scratch_shapes=[
                pltpu.VMEM((3 * SIDE, seg_rows, seg_rows), jnp.bfloat16),
                pltpu.VMEM((HALVES, 2, 2, SIDE) + panel, jnp.bfloat16),
                pltpu.VMEM((HALVES, DIAG_ACC + 1) + panel, jnp.float32),
                pltpu.VMEM((HALVES, SIDE + 1) + panel, jnp.float32),
                pltpu.VMEM((HALVES, 2, SIDE) + panel, jnp.float32),
                pltpu.VMEM((HALVES,) + panel, jnp.float32),
                pltpu.VMEM((HALVES,) + panel, jnp.float32),
                dma((3 * SIDE,)),
                dma((HALVES, 5, SIDE)),
                dma((HALVES, 2, SIDE)),
                dma((HALVES, 2, SIDE)),
                dma((HALVES, 2 * SIDE)),
                dma((HALVES, SIDE + 1)),
                dma((HALVES, 2, SIDE)),
            ],
            compiler_params=pltpu.CompilerParams(
                collective_id=0, has_side_effects=True, vmem_limit_bytes=67_000_000),
        )(h_slab[0, 0], h_diag[0], vec_occ.T, vec_virt.T)
        return filt_occ.T, filt_virt.T

    return jax.shard_map(local_filter, mesh=mesh, in_specs=(slab_spec, diag_spec, vec_spec, vec_spec), out_specs=(vec_spec, vec_spec), check_vma=False)
```

```python
import jax
import jax.numpy as jnp
from jax import lax
from jax.experimental import pallas as pl
from jax.experimental.pallas import tpu as pltpu
from jax.sharding import PartitionSpec as P

FILTER_STEPS = 3
CEN_OCC = 0.5
CEN_VIRT = -0.5
HALF_WIDTH = 1.5
SIDE = 4
HALVES = 2
UNITS = FILTER_STEPS * HALVES
EARLY = 2
CHUNKS = 2
MESH = pl.DeviceIdType.MESH
NN = (((1,), (0,)), ((), ()))
NT = (((1,), (1,)), ((), ()))


def filter_kernel(slab_hbm, strip_hbm, occ_ref, virt_ref, out_occ, out_virt,
                  mat, vec, acc, strip_acc, red, col, cur, prev,
                  mat_sem, vec_send, vec_recv, colvec_recv, acc_send, red_recv, col_recv):
    seg_rows = cur.shape[-1]
    n_vecs = cur.shape[1]
    part = n_vecs // CHUNKS

    def rows_of(q):
        return pl.ds(q * part, part)

    def half_rows(h, q):
        return pl.ds(pl.multiple_of(h * n_vecs + q * part, part), part)

    def half_of(h):
        return pl.ds(pl.multiple_of(h * n_vecs, n_vecs), n_vecs)

    kpt = lax.axis_index("kpt")
    c = lax.axis_index("col")
    r = lax.axis_index("row")
    is_diag = r == c
    lower = r > c
    upper = r < c
    chip = r // 2
    core = r % 2
    partner = r + 1 - 2 * core
    same_chip = (c // 2) == chip
    far0 = 2 * (1 - chip)
    col_peers = (partner, far0, far0 + 1)
    diag_dev = (kpt, c, c)

    def seg_order(i):
        ahead = jnp.where(c == 1, jnp.where(i < 2, 3 - i, i - 2), jnp.where(i < 2, i, 5 - i))
        return jnp.where(c == 0, 3 - i, jnp.where(c == 3, i, ahead))

    def goes_right(cc, seg):
        return (seg < 2) | (r <= cc)

    def goes_left(cc, seg):
        return ~((r == 3) & (cc == 3) & (seg < 2))

    def sends(seg):
        return jnp.where(seg > c, goes_right(c, seg), goes_left(c, seg)) & (seg != c)

    def from_left(seg):
        return (c > 0) & goes_right(c - 1, seg)

    def from_right(seg):
        return (c < 3) & goes_left(c + 1, seg)

    def incoming(seg):
        return jnp.where(seg > c, from_left(seg), from_right(seg))

    def row_copy(h, b, seg, way, q):
        return pltpu.make_async_remote_copy(
            src_ref=vec.at[b, 0, seg, half_rows(h, q)], dst_ref=vec.at[b, 0, seg, half_rows(h, q)],
            send_sem=vec_send.at[h, way, seg, q], recv_sem=vec_recv.at[h, b, seg, q],
            device_id=(kpt, c + 1 - 2 * way, r), device_id_type=MESH)

    def col_copy(h, b, seg, peer, q):
        return pltpu.make_async_remote_copy(
            src_ref=vec.at[b, 0, seg, half_rows(h, q)], dst_ref=vec.at[b, 1, seg, half_rows(h, q)],
            send_sem=vec_send.at[h, 2 + peer, seg, q], recv_sem=colvec_recv.at[h, b, seg, q],
            device_id=(kpt, c, col_peers[peer]), device_id_type=MESH)

    def red_copy(h, seg, q):
        step = jnp.where(seg > c, 1, -1)
        slot = jnp.where(seg == c - 1, SIDE, seg)
        return pltpu.make_async_remote_copy(
            src_ref=acc.at[h, seg, rows_of(q)], dst_ref=red.at[h, slot, rows_of(q)],
            send_sem=acc_send.at[h, seg, q], recv_sem=red_recv.at[h, slot, q],
            device_id=(kpt, c + step, r), device_id_type=MESH)

    def sum_copy(h, seg, slot, dev, q):
        return pltpu.make_async_remote_copy(
            src_ref=acc.at[h, SIDE + seg, rows_of(q)], dst_ref=col.at[h, slot, seg, rows_of(q)],
            send_sem=acc_send.at[h, SIDE + seg, q], recv_sem=col_recv.at[h, slot, seg, q],
            device_id=dev, device_id_type=MESH)

    def send_row(h, b, seg, left_ok, right_ok, q):
        @pl.when((c < 3) & right_ok)
        def _():
            row_copy(h, b, seg, 0, q).start()

        @pl.when((c > 0) & left_ok)
        def _():
            row_copy(h, b, seg, 1, q).start()

    def send_col(h, b, seg, q):
        for peer in range(3):
            @pl.when(is_diag & ((col_peers[peer] > c) | (seg >= 2)))
            def _():
                col_copy(h, b, seg, peer, q).start()

    def wait_vec_sends(h, b):
        def each(seg, carry):
            for q in range(CHUNKS):
                @pl.when((c < 3) & (seg <= c))
                def _():
                    row_copy(h, b, seg, 0, q).wait_send()

                @pl.when((c > 0) & (seg >= c))
                def _():
                    row_copy(h, b, seg, 1, q).wait_send()

                for peer in range(3):
                    @pl.when(is_diag & ((col_peers[peer] > c) | (seg >= 2)))
                    def _():
                        col_copy(h, b, seg, peer, q).wait_send()
            return carry

        lax.fori_loop(0, SIDE, each, 0)

    def wait_acc_sends(h):
        def each(seg, carry):
            for q in range(CHUNKS):
                @pl.when(sends(seg))
                def _():
                    red_copy(h, seg, q).wait_send()

                @pl.when(~is_diag & (lower | (seg >= 2)))
                def _():
                    sum_copy(h, seg, 0, diag_dev, q).wait_send()
            return carry

        lax.fori_loop(0, SIDE, each, 0)

    def wait_colvec(h, b, seg):
        for q in range(CHUNKS):
            col_copy(h, b, seg, 0, q).wait_recv()

    def send_sum(h, seg):
        for q in range(CHUNKS):
            @pl.when(same_chip)
            def _():
                sum_copy(h, seg, 0, diag_dev, q).start()

            @pl.when(~same_chip & (seg % 2 != core))
            def _():
                sum_copy(h, seg, 0, (kpt, c, partner), q).start()

    def combine_sums(h):
        def each(i, carry):
            seg = 2 * (1 - i) + core
            for q in range(CHUNKS):
                sum_copy(h, seg, 0, diag_dev, q).wait_recv()
                acc[h, SIDE + seg, rows_of(q)] += col[h, 0, seg, rows_of(q)]
                sum_copy(h, seg, 1, diag_dev, q).start()
            return carry

        @pl.when(~same_chip)
        def _():
            lax.fori_loop(0, jnp.where(lower, 2, 1), each, 0)

    def column_total(h, start, stop):
        def each(i, carry):
            seg = seg_order(i)
            near = (partner > c) | (seg >= 2)
            far = (far0 > c) | (seg >= 2)
            for q in range(CHUNKS):
                @pl.when(near)
                def _():
                    sum_copy(h, seg, 0, diag_dev, q).wait_recv()
                    acc[h, seg, rows_of(q)] += col[h, 0, seg, rows_of(q)]

                @pl.when(far)
                def _():
                    sum_copy(h, seg, 1, diag_dev, q).wait_recv()
                    acc[h, seg, rows_of(q)] += col[h, 1, seg, rows_of(q)]
                start_sum(h, seg, q)
            return carry

        lax.fori_loop(start, stop, each, 0)

    def arrived(h, seg, slot, q):
        pltpu.make_async_remote_copy(
            src_ref=acc.at[h, seg, rows_of(q)], dst_ref=red.at[h, slot, rows_of(q)],
            send_sem=acc_send.at[h, seg, q], recv_sem=red_recv.at[h, slot, q],
            device_id=diag_dev, device_id_type=MESH).wait_recv()
        acc[h, seg, rows_of(q)] += red[h, slot, rows_of(q)]

    def relay(h, seg):
        @pl.when(sends(seg) & incoming(seg))
        def _():
            for q in range(CHUNKS):
                arrived(h, seg, seg, q)
                red_copy(h, seg, q).start()

    def start_sum(h, seg, q):
        @pl.when(sends(seg) & ~incoming(seg))
        def _():
            red_copy(h, seg, q).start()

    def product(left, right, dims):
        return lax.dot_general(left, right, dims, preferred_element_type=jnp.float32)

    first_half = jnp.where(c == 0, 0, 1)

    def slab_load(half, seg):
        rows = pl.ds(pl.multiple_of(half * seg_rows, seg_rows), seg_rows)
        return pltpu.make_async_copy(
            slab_hbm.at[rows, pl.ds(pl.multiple_of(seg * seg_rows, seg_rows), seg_rows)],
            mat.at[seg, rows], mat_sem.at[half, seg])

    def strip_load(seg):
        return pltpu.make_async_copy(
            strip_hbm.at[:, pl.ds(pl.multiple_of(seg * seg_rows, seg_rows), seg_rows)],
            mat.at[seg, pl.ds(2 * seg_rows, seg_rows)], mat_sem.at[2, seg])

    def strip_terms(k, b):
        strip_acc[...] = jnp.zeros_like(strip_acc)

        def each(seg, carry):
            @pl.when(k == 1)
            def _():
                strip_load(seg).wait()
            strip_acc[...] += product(vec[b, 0, seg], mat[seg, 2 * seg_rows:], NT)
            return carry

        lax.fori_loop(0, SIDE, each, 0)

    def take_piece(k, h, b, seg):
        @pl.when(upper)
        def _():
            @pl.when((k == 0) & ((c < 3) | (seg > 0)))
            def _():
                for half in range(2):
                    slab_load(half, seg).wait()
            both = product(vec[b, 0, seg, half_of(h)], mat[seg, :2 * seg_rows], NT)
            for i in range(2):
                acc[h, SIDE + 2 + i] += both[:, i * seg_rows:(i + 1) * seg_rows]

        @pl.when(lower & (seg < 2))
        def _():
            @pl.when(k == 0)
            def _():
                for j in range(SIDE):
                    slab_load(seg, j).wait()

                @pl.when(seg == first_half)
                def _():
                    for j in range(SIDE):
                        slab_load(1 - first_half, j).start()
            rows = pl.ds(pl.multiple_of(seg * seg_rows, seg_rows), seg_rows)
            for j in range(SIDE):
                acc[h, SIDE + j] += product(vec[b, 0, seg, half_of(h)], mat[j, rows], NN)

    def upper_row_terms(h, b):
        def each(i, carry):
            seg = seg_order(i)
            acc[h, seg] = (product(vec[b, 1, 2, half_of(h)], mat[seg, :seg_rows], NN)
                           + product(vec[b, 1, 3, half_of(h)], mat[seg, seg_rows:2 * seg_rows], NN))

            @pl.when(i < EARLY)
            def _():
                for q in range(CHUNKS):
                    start_sum(h, seg, q)
            return carry

        lax.fori_loop(0, SIDE, each, 0)

    def lower_row_terms(h, b):
        def each(i, carry):
            seg = (i + c) % SIDE

            @pl.when(i > 0)
            def _():
                wait_colvec(h, b, seg)
            both = product(vec[b, 1, seg, half_of(h)], mat[seg, :2 * seg_rows], NT)
            for half in range(2):
                acc[h, half] += both[:, half * seg_rows:(half + 1) * seg_rows]
            return carry

        lax.fori_loop(0, SIDE, each, 0)

    def finish(k, h, b, next_b):
        wait_vec_sends(h, b)

        for q in range(CHUNKS):
            @pl.when(from_left(c))
            def _():
                arrived(h, c, c, q)

            @pl.when(from_right(c))
            def _():
                arrived(h, c, SIDE, q)

        center = jnp.where(h == 0, CEN_OCC, CEN_VIRT)
        applied = acc[h, c] + strip_acc[half_of(h)]
        scaled = (applied - center * cur[h]) * (1.0 / HALF_WIDTH)
        first = k < HALVES
        nxt = jnp.where(first, scaled, 2.0 * scaled - prev[h])
        prev[h] = cur[h]
        cur[h] = nxt

        @pl.when(k + HALVES < UNITS)
        def _():
            vec[next_b, 0, c, half_of(h)] = nxt.astype(jnp.bfloat16)
            for q in range(CHUNKS):
                send_row(h, next_b, c, True, True, q)
                send_col(h, next_b, c, q)

    barrier = pltpu.get_barrier_semaphore()

    @pl.when(c > 0)
    def _():
        pl.semaphore_signal(barrier, inc=1, device_id=(kpt, c - 1, r), device_id_type=MESH)

    @pl.when(c < 3)
    def _():
        pl.semaphore_signal(barrier, inc=1, device_id=(kpt, c + 1, r), device_id_type=MESH)

    for peer in range(3):
        pl.semaphore_signal(barrier, inc=1, device_id=(kpt, c, col_peers[peer]), device_id_type=MESH)

    def load_block(i, carry):
        seg = (c + i) % SIDE

        @pl.when(upper)
        def _():
            for half in range(2):
                slab_load(half, seg).start()

        @pl.when(lower)
        def _():
            slab_load(first_half, seg).start()
        return carry

    lax.fori_loop(0, SIDE, load_block, 0)
    for h, src in enumerate((occ_ref, virt_ref)):
        cur[h] = src[...]
        prev[h] = jnp.zeros_like(src)
        vec[0, 0, c, half_of(h)] = src[...].astype(jnp.bfloat16)
    pl.semaphore_wait(barrier, 3 + (c > 0).astype(jnp.int32) + (c < 3).astype(jnp.int32))
    for q in range(CHUNKS):
        send_row(0, 0, c, True, True, q)
        send_col(0, 0, c, q)

    def slot(k, carry):
        h = k % 2
        b = (k // 2) % 2
        last = k - 1
        lh = (k + 1) % 2
        lb = ((k + 1) // 2 + 1) % 2
        live = k < UNITS
        older = k >= 1

        @pl.when(live)
        def _():
            @pl.when(k >= HALVES)
            def _():
                wait_acc_sends(h)

            def clear(i, cc):
                acc[h, i] = jnp.zeros(acc.shape[2:], acc.dtype)
                return cc

            lax.fori_loop(0, 2 * SIDE, clear, 0)

        def arrivals(d, cc):
            for q in range(CHUNKS):
                for s in range(2):
                    seg = c + (2 * s - 1) * d

                    @pl.when(live & (seg >= 0) & (seg < SIDE) & (d > 0))
                    def _():
                        row_copy(h, b, seg, 0, q).wait_recv()
                        send_row(h, b, seg, s == 1, s == 0, q)
                        send_col(h, b, seg, q)

            @pl.when(older & is_diag & (c >= 2) & (d == 1))
            def _():
                column_total(lh, 0, SIDE)

            def hop(i):
                @pl.when(older & (c > 0) & (c < 3) & (i >= 0) & (i < 3))
                def _():
                    relay(lh, jnp.where(c == 1, jnp.where(i == 2, 0, 3 - i), jnp.where(i == 2, 3, i)))

            hop(d - 1 - 5 * (d == 3))

            @pl.when((k == 0) & (d == 2))
            def _():
                for q in range(CHUNKS):
                    send_row(1, 0, c, True, True, q)
                    send_col(1, 0, c, q)

            def use(s, ccc):
                seg = c + (2 * s - 1) * d

                @pl.when(live & (seg >= 0) & (seg < SIDE) & ((d > 0) | (s == 0)))
                def _():
                    take_piece(k, h, b, seg)
                return ccc

            lax.fori_loop(0, 2, use, 0)

            hop(jnp.where(d == 2, 2, -1))

            @pl.when(live & lower & (d == jnp.where(c == 2, 2, 1)))
            def _():
                wait_colvec(h, b, c)

                def each(i, ccc):
                    send_sum(h, seg_order(i))
                    return ccc

                lax.fori_loop(0, SIDE, each, 0)

            @pl.when(live & lower & (d == 2))
            def _():
                combine_sums(h)

            @pl.when(live & upper & (d == 2))
            def _():
                wait_colvec(h, b, 2)
                wait_colvec(h, b, 3)

                @pl.when((k == 0) & (c == 3))
                def _():
                    for half in range(2):
                        slab_load(half, 0).wait()
                upper_row_terms(h, b)
            return cc

        lax.fori_loop(0, SIDE, arrivals, 0)

        @pl.when(k == 0)
        def _():
            for j in range(SIDE):
                strip_load(j).start()

        @pl.when(live & upper)
        def _():
            send_sum(h, 2)
            send_sum(h, 3)

        @pl.when(live & lower)
        def _():
            lower_row_terms(h, b)

        @pl.when(live & is_diag & (c < 2))
        def _():
            column_total(h, 0, 2)

        @pl.when(live & (h == 1))
        def _():
            strip_terms(k, b)

        @pl.when(older)
        def _():
            finish(last, lh, lb, 1 - lb)

        @pl.when(live & ~is_diag)
        def _():
            def each(i, cc):
                for q in range(CHUNKS):
                    start_sum(h, seg_order(i), q)
                return cc

            lax.fori_loop(jnp.where(upper, EARLY, 0), SIDE, each, 0)

        @pl.when(live & upper)
        def _():
            combine_sums(h)

        @pl.when(live & is_diag & (c < 2))
        def _():
            column_total(h, 2, SIDE)
        return carry

    lax.fori_loop(0, UNITS + 1, slot, 0)
    for h in range(HALVES):
        wait_acc_sends(h)
    out_occ[...] = cur[0]
    out_virt[...] = cur[1]


def solution(mesh):
    slab_spec = P(("kpt", "row"), "col", None, None)
    diag_spec = P(("kpt", "row"), "col", None)
    vec_spec = P(("kpt", "row", "col"), None)

    def local_filter(h_slab, h_diag, vec_occ, vec_virt):
        seg_rows, n_vecs = vec_occ.shape
        panel = (n_vecs, seg_rows)
        out = jax.ShapeDtypeStruct(panel, jnp.float32)
        vmem = pl.BlockSpec(memory_space=pltpu.VMEM)
        hbm = pl.BlockSpec(memory_space=pl.ANY)
        dma = pltpu.SemaphoreType.DMA
        filt_occ, filt_virt = pl.pallas_call(
            filter_kernel,
            out_shape=(out, out),
            in_specs=[hbm, hbm, vmem, vmem],
            out_specs=(vmem, vmem),
            scratch_shapes=[
                pltpu.VMEM((SIDE, 3 * seg_rows, seg_rows), jnp.bfloat16),
                pltpu.VMEM((2, 2, SIDE, HALVES * n_vecs, seg_rows), jnp.bfloat16),
                pltpu.VMEM((HALVES, 2 * SIDE) + panel, jnp.float32),
                pltpu.VMEM((HALVES * n_vecs, seg_rows), jnp.float32),
                pltpu.VMEM((HALVES, SIDE + 1) + panel, jnp.float32),
                pltpu.VMEM((HALVES, 2, SIDE) + panel, jnp.float32),
                pltpu.VMEM((HALVES,) + panel, jnp.float32),
                pltpu.VMEM((HALVES,) + panel, jnp.float32),
                dma((3, SIDE)),
                dma((HALVES, 5, SIDE, CHUNKS)),
                dma((HALVES, 2, SIDE, CHUNKS)),
                dma((HALVES, 2, SIDE, CHUNKS)),
                dma((HALVES, 2 * SIDE, CHUNKS)),
                dma((HALVES, SIDE + 1, CHUNKS)),
                dma((HALVES, 2, SIDE, CHUNKS)),
            ],
            compiler_params=pltpu.CompilerParams(
                collective_id=0, has_side_effects=True, vmem_limit_bytes=67_000_000),
        )(h_slab[0, 0], h_diag[0], vec_occ.T, vec_virt.T)
        return filt_occ.T, filt_virt.T

    return jax.shard_map(local_filter, mesh=mesh, in_specs=(slab_spec, diag_spec, vec_spec, vec_spec), out_specs=(vec_spec, vec_spec), check_vma=False)
```

```python
import jax
import jax.numpy as jnp
from jax import lax
from jax.experimental import pallas as pl
from jax.experimental.pallas import tpu as pltpu
from jax.sharding import PartitionSpec as P

FILTER_STEPS = 3
CEN_OCC = 0.5
CEN_VIRT = -0.5
HALF_WIDTH = 1.5
SIDE = 4
HALVES = 2
UNITS = FILTER_STEPS * HALVES
EARLY = 2
CHUNKS = 2
MESH = pl.DeviceIdType.MESH
NN = (((1,), (0,)), ((), ()))
NT = (((1,), (1,)), ((), ()))


def filter_kernel(slab_hbm, strip_hbm, occ_ref, virt_ref, out,
                  mat, vec, acc, strip_acc, red, col, cur, prev,
                  mat_sem, vec_send, vec_recv, colvec_recv, acc_send, red_recv, col_recv):
    seg_rows = cur.shape[-1]
    n_vecs = cur.shape[1]
    part = n_vecs // CHUNKS

    def rows_of(q):
        return pl.ds(q * part, part)

    def half_rows(h, q):
        return pl.ds(pl.multiple_of(h * n_vecs + q * part, part), part)

    def half_of(h):
        return pl.ds(pl.multiple_of(h * n_vecs, n_vecs), n_vecs)

    kpt = lax.axis_index("kpt")
    c = lax.axis_index("col")
    r = lax.axis_index("row")
    is_diag = r == c
    lower = r > c
    upper = r < c
    chip = r // 2
    core = r % 2
    partner = r + 1 - 2 * core
    same_chip = (c // 2) == chip
    far0 = 2 * (1 - chip)
    col_peers = (partner, far0, far0 + 1)
    diag_dev = (kpt, c, c)

    def seg_order(i):
        ahead = jnp.where(c == 1, jnp.where(i < 2, 3 - i, i - 2), jnp.where(i < 2, i, 5 - i))
        return jnp.where(c == 0, 3 - i, jnp.where(c == 3, i, ahead))

    def goes_right(cc, seg):
        return (seg < 2) | (r <= cc)

    def goes_left(cc, seg):
        return ~((r == 3) & (cc == 3) & (seg < 2))

    def sends(seg):
        return jnp.where(seg > c, goes_right(c, seg), goes_left(c, seg)) & (seg != c)

    def from_left(seg):
        return (c > 0) & goes_right(c - 1, seg)

    def from_right(seg):
        return (c < 3) & goes_left(c + 1, seg)

    def incoming(seg):
        return jnp.where(seg > c, from_left(seg), from_right(seg))

    def row_copy(h, b, seg, way, q):
        return pltpu.make_async_remote_copy(
            src_ref=vec.at[b, 0, seg, half_rows(h, q)], dst_ref=vec.at[b, 0, seg, half_rows(h, q)],
            send_sem=vec_send.at[h, way, seg, q], recv_sem=vec_recv.at[h, b, seg, q],
            device_id=(kpt, c + 1 - 2 * way, r), device_id_type=MESH)

    def col_copy(h, b, seg, peer, q):
        return pltpu.make_async_remote_copy(
            src_ref=vec.at[b, 0, seg, half_rows(h, q)], dst_ref=vec.at[b, 1, seg, half_rows(h, q)],
            send_sem=vec_send.at[h, 2 + peer, seg, q], recv_sem=colvec_recv.at[h, b, seg, q],
            device_id=(kpt, c, col_peers[peer]), device_id_type=MESH)

    def red_copy(h, seg, q):
        step = jnp.where(seg > c, 1, -1)
        slot = jnp.where(seg == c - 1, SIDE, seg)
        return pltpu.make_async_remote_copy(
            src_ref=acc.at[h, seg, rows_of(q)], dst_ref=red.at[h, slot, rows_of(q)],
            send_sem=acc_send.at[h, seg, q], recv_sem=red_recv.at[h, slot, q],
            device_id=(kpt, c + step, r), device_id_type=MESH)

    def sum_copy(h, seg, slot, dev, q):
        return pltpu.make_async_remote_copy(
            src_ref=acc.at[h, SIDE + seg, rows_of(q)], dst_ref=col.at[h, slot, seg, rows_of(q)],
            send_sem=acc_send.at[h, SIDE + seg, q], recv_sem=col_recv.at[h, slot, seg, q],
            device_id=dev, device_id_type=MESH)

    def send_row(h, b, seg, left_ok, right_ok, q):
        @pl.when((c < 3) & right_ok)
        def _():
            row_copy(h, b, seg, 0, q).start()

        @pl.when((c > 0) & left_ok)
        def _():
            row_copy(h, b, seg, 1, q).start()

    def send_col(h, b, seg, q):
        for peer in range(3):
            @pl.when(is_diag & ((col_peers[peer] > c) | (seg >= 2)))
            def _():
                col_copy(h, b, seg, peer, q).start()

    def wait_vec_sends(h, b):
        def each(seg, carry):
            for q in range(CHUNKS):
                @pl.when((c < 3) & (seg <= c))
                def _():
                    row_copy(h, b, seg, 0, q).wait_send()

                @pl.when((c > 0) & (seg >= c))
                def _():
                    row_copy(h, b, seg, 1, q).wait_send()

                for peer in range(3):
                    @pl.when(is_diag & ((col_peers[peer] > c) | (seg >= 2)))
                    def _():
                        col_copy(h, b, seg, peer, q).wait_send()
            return carry

        lax.fori_loop(0, SIDE, each, 0)

    def wait_acc_sends(h):
        def each(seg, carry):
            for q in range(CHUNKS):
                @pl.when(sends(seg))
                def _():
                    red_copy(h, seg, q).wait_send()

                @pl.when(~is_diag & (lower | (seg >= 2)))
                def _():
                    sum_copy(h, seg, 0, diag_dev, q).wait_send()
            return carry

        lax.fori_loop(0, SIDE, each, 0)

    def wait_colvec(h, b, seg):
        for q in range(CHUNKS):
            col_copy(h, b, seg, 0, q).wait_recv()

    def send_sum(h, seg):
        for q in range(CHUNKS):
            @pl.when(same_chip)
            def _():
                sum_copy(h, seg, 0, diag_dev, q).start()

            @pl.when(~same_chip & (seg % 2 != core))
            def _():
                sum_copy(h, seg, 0, (kpt, c, partner), q).start()

    def combine_sums(h):
        def each(i, carry):
            seg = 2 * (1 - i) + core
            for q in range(CHUNKS):
                sum_copy(h, seg, 0, diag_dev, q).wait_recv()
                acc[h, SIDE + seg, rows_of(q)] += col[h, 0, seg, rows_of(q)]
                sum_copy(h, seg, 1, diag_dev, q).start()
            return carry

        @pl.when(~same_chip)
        def _():
            lax.fori_loop(0, jnp.where(lower, 2, 1), each, 0)

    def column_total(h, start, stop):
        def each(i, carry):
            seg = seg_order(i)
            near = (partner > c) | (seg >= 2)
            far = (far0 > c) | (seg >= 2)
            for q in range(CHUNKS):
                @pl.when(near)
                def _():
                    sum_copy(h, seg, 0, diag_dev, q).wait_recv()
                    acc[h, seg, rows_of(q)] += col[h, 0, seg, rows_of(q)]

                @pl.when(far)
                def _():
                    sum_copy(h, seg, 1, diag_dev, q).wait_recv()
                    acc[h, seg, rows_of(q)] += col[h, 1, seg, rows_of(q)]
                start_sum(h, seg, q)
            return carry

        lax.fori_loop(start, stop, each, 0)

    def arrived(h, seg, slot, q):
        pltpu.make_async_remote_copy(
            src_ref=acc.at[h, seg, rows_of(q)], dst_ref=red.at[h, slot, rows_of(q)],
            send_sem=acc_send.at[h, seg, q], recv_sem=red_recv.at[h, slot, q],
            device_id=diag_dev, device_id_type=MESH).wait_recv()
        acc[h, seg, rows_of(q)] += red[h, slot, rows_of(q)]

    def relay(h, seg):
        @pl.when(sends(seg) & incoming(seg))
        def _():
            for q in range(CHUNKS):
                arrived(h, seg, seg, q)
                red_copy(h, seg, q).start()

    def start_sum(h, seg, q):
        @pl.when(sends(seg) & ~incoming(seg))
        def _():
            red_copy(h, seg, q).start()

    def product(left, right, dims):
        return lax.dot_general(left, right, dims, preferred_element_type=jnp.float32)

    first_half = jnp.where(c == 0, 0, 1)

    def slab_load(half, seg):
        rows = pl.ds(pl.multiple_of(half * seg_rows, seg_rows), seg_rows)
        return pltpu.make_async_copy(
            slab_hbm.at[rows, pl.ds(pl.multiple_of(seg * seg_rows, seg_rows), seg_rows)],
            mat.at[seg, rows], mat_sem.at[half, seg])

    def strip_load(seg):
        return pltpu.make_async_copy(
            strip_hbm.at[:, pl.ds(pl.multiple_of(seg * seg_rows, seg_rows), seg_rows)],
            mat.at[seg, pl.ds(2 * seg_rows, seg_rows)], mat_sem.at[2, seg])

    def strip_terms(k, b, seg, first):
        @pl.when(k == 1)
        def _():
            strip_load(seg).wait()
        term = product(vec[b, 0, seg], mat[seg, 2 * seg_rows:], NT)
        strip_acc[...] = jnp.where(first, 0.0, strip_acc[...]) + term

    def take_piece(k, h, b, seg):
        @pl.when(upper)
        def _():
            @pl.when((k == 0) & ((c < 3) | (seg > 0)))
            def _():
                for half in range(2):
                    slab_load(half, seg).wait()
            both = product(vec[b, 0, seg, half_of(h)], mat[seg, :2 * seg_rows], NT)
            for i in range(2):
                acc[h, SIDE + 2 + i] += both[:, i * seg_rows:(i + 1) * seg_rows]

        @pl.when(lower & (seg < 2))
        def _():
            @pl.when(k == 0)
            def _():
                for j in range(SIDE):
                    slab_load(seg, j).wait()

                @pl.when(seg == first_half)
                def _():
                    for j in range(SIDE):
                        slab_load(1 - first_half, j).start()
            rows = pl.ds(pl.multiple_of(seg * seg_rows, seg_rows), seg_rows)
            for j in range(SIDE):
                acc[h, SIDE + j] += product(vec[b, 0, seg, half_of(h)], mat[j, rows], NN)

    def upper_row_terms(h, b):
        def each(i, carry):
            seg = seg_order(i)
            acc[h, seg] = (product(vec[b, 1, 2, half_of(h)], mat[seg, :seg_rows], NN)
                           + product(vec[b, 1, 3, half_of(h)], mat[seg, seg_rows:2 * seg_rows], NN))

            @pl.when(i < EARLY)
            def _():
                for q in range(CHUNKS):
                    start_sum(h, seg, q)
            return carry

        lax.fori_loop(0, SIDE, each, 0)

    def lower_row_terms(h, b):
        def each(i, carry):
            seg = (i + c) % SIDE

            @pl.when(i > 0)
            def _():
                wait_colvec(h, b, seg)
            both = product(vec[b, 1, seg, half_of(h)], mat[seg, :2 * seg_rows], NT)
            for half in range(2):
                acc[h, half] += both[:, half * seg_rows:(half + 1) * seg_rows]
            return carry

        lax.fori_loop(0, SIDE, each, 0)

    def finish(k, h, b, next_b):
        wait_vec_sends(h, b)

        for q in range(CHUNKS):
            @pl.when(from_left(c))
            def _():
                arrived(h, c, c, q)

            @pl.when(from_right(c))
            def _():
                arrived(h, c, SIDE, q)

        center = jnp.where(h == 0, CEN_OCC, CEN_VIRT)
        applied = acc[h, c] + strip_acc[half_of(h)]
        scaled = (applied - center * cur[h]) * (1.0 / HALF_WIDTH)
        first = k < HALVES
        nxt = jnp.where(first, scaled, 2.0 * scaled - prev[h])
        prev[h] = cur[h]
        cur[h] = nxt

        @pl.when(k + HALVES < UNITS)
        def _():
            vec[next_b, 0, c, half_of(h)] = nxt.astype(jnp.bfloat16)
            for q in range(CHUNKS):
                send_row(h, next_b, c, True, True, q)
                send_col(h, next_b, c, q)

    barrier = pltpu.get_barrier_semaphore()

    @pl.when(c > 0)
    def _():
        pl.semaphore_signal(barrier, inc=1, device_id=(kpt, c - 1, r), device_id_type=MESH)

    @pl.when(c < 3)
    def _():
        pl.semaphore_signal(barrier, inc=1, device_id=(kpt, c + 1, r), device_id_type=MESH)

    for peer in range(3):
        pl.semaphore_signal(barrier, inc=1, device_id=(kpt, c, col_peers[peer]), device_id_type=MESH)

    def load_block(i, carry):
        seg = (c + i) % SIDE

        @pl.when(upper)
        def _():
            for half in range(2):
                slab_load(half, seg).start()

        @pl.when(lower)
        def _():
            slab_load(first_half, seg).start()
        return carry

    lax.fori_loop(0, SIDE, load_block, 0)
    for h, src in enumerate((occ_ref, virt_ref)):
        cur[h] = src[...]
        prev[h] = jnp.zeros_like(src)
        vec[0, 0, c, half_of(h)] = src[...].astype(jnp.bfloat16)
    pl.semaphore_wait(barrier, 3 + (c > 0).astype(jnp.int32) + (c < 3).astype(jnp.int32))
    for q in range(CHUNKS):
        send_row(0, 0, c, True, True, q)
        send_col(0, 0, c, q)

    def slot(k, carry):
        h = k % 2
        b = (k // 2) % 2
        last = k - 1
        lh = (k + 1) % 2
        lb = ((k + 1) // 2 + 1) % 2
        live = k < UNITS
        older = k >= 1

        @pl.when(live)
        def _():
            @pl.when(k >= HALVES)
            def _():
                wait_acc_sends(h)

            def clear(i, cc):
                acc[h, i] = jnp.zeros(acc.shape[2:], acc.dtype)
                return cc

            lax.fori_loop(0, 2 * SIDE, clear, 0)

        def arrivals(d, cc):
            for s in (1, 0):
                for q in range(CHUNKS):
                    seg = c + (2 * s - 1) * d

                    @pl.when(live & (seg >= 0) & (seg < SIDE) & (d > 0))
                    def _():
                        row_copy(h, b, seg, 0, q).wait_recv()
                        send_row(h, b, seg, s == 1, s == 0, q)
                        send_col(h, b, seg, q)

            @pl.when(older & is_diag & (c >= 2) & (d == 1))
            def _():
                column_total(lh, 0, SIDE)

            def hop(i):
                @pl.when(older & (c > 0) & (c < 3) & (i >= 0) & (i < 3))
                def _():
                    relay(lh, jnp.where(c == 1, jnp.where(i == 2, 0, 3 - i), jnp.where(i == 2, 3, i)))

            hop(d - 1 - 5 * (d == 3))

            @pl.when((k == 0) & (d == 2))
            def _():
                for q in range(CHUNKS):
                    send_row(1, 0, c, True, True, q)
                    send_col(1, 0, c, q)

            def use(s, ccc):
                seg = c + (2 * s - 1) * d

                @pl.when(live & (seg >= 0) & (seg < SIDE) & ((d > 0) | (s == 0)))
                def _():
                    take_piece(k, h, b, seg)

                    @pl.when(h == 1)
                    def _():
                        strip_terms(k, b, seg, d == 0)
                return ccc

            lax.fori_loop(0, 2, use, 0)

            hop(jnp.where(d == 2, 2, -1))

            @pl.when(live & lower & (d == jnp.where(c == 2, 2, 1)))
            def _():
                wait_colvec(h, b, c)

                def each(i, ccc):
                    send_sum(h, seg_order(i))
                    return ccc

                lax.fori_loop(0, SIDE, each, 0)

            @pl.when(live & lower & (d == 2))
            def _():
                combine_sums(h)

            @pl.when(live & upper & (d == 2))
            def _():
                wait_colvec(h, b, 2)
                wait_colvec(h, b, 3)

                @pl.when((k == 0) & (c == 3))
                def _():
                    for half in range(2):
                        slab_load(half, 0).wait()
                upper_row_terms(h, b)
            return cc

        lax.fori_loop(0, SIDE, arrivals, 0)

        @pl.when(k == 0)
        def _():
            for j in range(SIDE):
                strip_load(j).start()

        @pl.when(live & upper)
        def _():
            send_sum(h, 2)
            send_sum(h, 3)

        @pl.when(live & lower)
        def _():
            lower_row_terms(h, b)

        @pl.when(live & is_diag & (c == 0))
        def _():
            column_total(h, 0, 2)

        @pl.when(older)
        def _():
            finish(last, lh, lb, 1 - lb)

        @pl.when(live & ~is_diag)
        def _():
            def each(i, cc):
                for q in range(CHUNKS):
                    start_sum(h, seg_order(i), q)
                return cc

            lax.fori_loop(jnp.where(upper, EARLY, 0), SIDE, each, 0)

        @pl.when(live & upper)
        def _():
            combine_sums(h)

        @pl.when(live & is_diag & (c < 2))
        def _():
            column_total(h, jnp.where(c == 0, 2, 0), SIDE)
        return carry

    lax.fori_loop(0, UNITS + 1, slot, 0)
    for h in range(HALVES):
        wait_acc_sends(h)
    for h in range(HALVES):
        out[h * n_vecs:(h + 1) * n_vecs] = cur[h]


def solution(mesh):
    slab_spec = P(("kpt", "row"), "col", None, None)
    diag_spec = P(("kpt", "row"), "col", None)
    vec_spec = P(("kpt", "row", "col"), None)

    def local_filter(h_slab, h_diag, vec_occ, vec_virt):
        seg_rows, n_vecs = vec_occ.shape
        panel = (n_vecs, seg_rows)
        vmem = pl.BlockSpec(memory_space=pltpu.VMEM)
        hbm = pl.BlockSpec(memory_space=pl.ANY)
        dma = pltpu.SemaphoreType.DMA
        both = pl.pallas_call(
            filter_kernel,
            out_shape=jax.ShapeDtypeStruct((HALVES * n_vecs, seg_rows), jnp.float32),
            in_specs=[hbm, hbm, vmem, vmem],
            out_specs=vmem,
            scratch_shapes=[
                pltpu.VMEM((SIDE, 3 * seg_rows, seg_rows), jnp.bfloat16),
                pltpu.VMEM((2, 2, SIDE, HALVES * n_vecs, seg_rows), jnp.bfloat16),
                pltpu.VMEM((HALVES, 2 * SIDE) + panel, jnp.float32),
                pltpu.VMEM((HALVES * n_vecs, seg_rows), jnp.float32),
                pltpu.VMEM((HALVES, SIDE + 1) + panel, jnp.float32),
                pltpu.VMEM((HALVES, 2, SIDE) + panel, jnp.float32),
                pltpu.VMEM((HALVES,) + panel, jnp.float32),
                pltpu.VMEM((HALVES,) + panel, jnp.float32),
                dma((3, SIDE)),
                dma((HALVES, 5, SIDE, CHUNKS)),
                dma((HALVES, 2, SIDE, CHUNKS)),
                dma((HALVES, 2, SIDE, CHUNKS)),
                dma((HALVES, 2 * SIDE, CHUNKS)),
                dma((HALVES, SIDE + 1, CHUNKS)),
                dma((HALVES, 2, SIDE, CHUNKS)),
            ],
            compiler_params=pltpu.CompilerParams(
                collective_id=0, has_side_effects=True, vmem_limit_bytes=67_000_000),
        )(h_slab[0, 0], h_diag[0], vec_occ.T, vec_virt.T)
        return both[:n_vecs].T, both[n_vecs:].T

    return jax.shard_map(local_filter, mesh=mesh, in_specs=(slab_spec, diag_spec, vec_spec, vec_spec), out_specs=(vec_spec, vec_spec), check_vma=False)
```

```python
import jax
import jax.numpy as jnp
from jax import lax
from jax.experimental import pallas as pl
from jax.experimental.pallas import tpu as pltpu
from jax.sharding import PartitionSpec as P

FILTER_STEPS = 3
CEN_OCC = 0.5
CEN_VIRT = -0.5
HALF_WIDTH = 1.5
SIDE = 4
HALVES = 2
UNITS = FILTER_STEPS * HALVES
EARLY = 2
CHUNKS = 2
MESH = pl.DeviceIdType.MESH
NN = (((1,), (0,)), ((), ()))
NT = (((1,), (1,)), ((), ()))


def filter_kernel(slab_hbm, strip_hbm, occ_ref, virt_ref, out,
                  mat, vec, acc, strip_acc, red, col, cur, prev,
                  mat_sem, vec_send, vec_recv, colvec_recv, acc_send, red_recv, col_recv):
    seg_rows = cur.shape[-1]
    n_vecs = cur.shape[1]
    part = n_vecs // CHUNKS

    def rows_of(q):
        return pl.ds(q * part, part)

    def half_rows(h, q):
        return pl.ds(pl.multiple_of(h * n_vecs + q * part, part), part)

    def half_of(h):
        return pl.ds(pl.multiple_of(h * n_vecs, n_vecs), n_vecs)

    kpt = lax.axis_index("kpt")
    c = lax.axis_index("col")
    r = lax.axis_index("row")
    is_diag = r == c
    lower = r > c
    upper = r < c
    chip = r // 2
    core = r % 2
    partner = r + 1 - 2 * core
    same_chip = (c // 2) == chip
    far0 = 2 * (1 - chip)
    col_peers = (partner, far0, far0 + 1)
    diag_dev = (kpt, c, c)

    def seg_order(i):
        ahead = jnp.where(c == 1, jnp.where(i < 2, 3 - i, i - 2), jnp.where(i < 2, i, 5 - i))
        return jnp.where(c == 0, 3 - i, jnp.where(c == 3, i, ahead))

    def goes_right(cc, seg):
        return (seg < 2) | (r <= cc)

    def goes_left(cc, seg):
        return ~((r == 3) & (cc == 3) & (seg < 2))

    def sends(seg):
        return jnp.where(seg > c, goes_right(c, seg), goes_left(c, seg)) & (seg != c)

    def from_left(seg):
        return (c > 0) & goes_right(c - 1, seg)

    def from_right(seg):
        return (c < 3) & goes_left(c + 1, seg)

    def incoming(seg):
        return jnp.where(seg > c, from_left(seg), from_right(seg))

    def row_copy(h, b, seg, way, q):
        return pltpu.make_async_remote_copy(
            src_ref=vec.at[b, 0, seg, half_rows(h, q)], dst_ref=vec.at[b, 0, seg, half_rows(h, q)],
            send_sem=vec_send.at[h, way, seg, q], recv_sem=vec_recv.at[h, b, seg, q],
            device_id=(kpt, c + 1 - 2 * way, r), device_id_type=MESH)

    def col_copy(h, b, seg, peer, q):
        return pltpu.make_async_remote_copy(
            src_ref=vec.at[b, 0, seg, half_rows(h, q)], dst_ref=vec.at[b, 1, seg, half_rows(h, q)],
            send_sem=vec_send.at[h, 2 + peer, seg, q], recv_sem=colvec_recv.at[h, b, seg, q],
            device_id=(kpt, c, col_peers[peer]), device_id_type=MESH)

    def red_copy(h, seg, q):
        step = jnp.where(seg > c, 1, -1)
        slot = jnp.where(seg == c - 1, SIDE, seg)
        return pltpu.make_async_remote_copy(
            src_ref=acc.at[h, seg, rows_of(q)], dst_ref=red.at[h, slot, rows_of(q)],
            send_sem=acc_send.at[h, seg, q], recv_sem=red_recv.at[h, slot, q],
            device_id=(kpt, c + step, r), device_id_type=MESH)

    def sum_copy(h, seg, slot, dev, q):
        return pltpu.make_async_remote_copy(
            src_ref=acc.at[h, SIDE + seg, rows_of(q)], dst_ref=col.at[h, slot, seg, rows_of(q)],
            send_sem=acc_send.at[h, SIDE + seg, q], recv_sem=col_recv.at[h, slot, seg, q],
            device_id=dev, device_id_type=MESH)

    def send_row(h, b, seg, left_ok, right_ok, q):
        @pl.when((c < 3) & right_ok)
        def _():
            row_copy(h, b, seg, 0, q).start()

        @pl.when((c > 0) & left_ok)
        def _():
            row_copy(h, b, seg, 1, q).start()

    def send_col(h, b, seg, q):
        for peer in range(3):
            @pl.when(is_diag & ((col_peers[peer] > c) | (seg >= 2)))
            def _():
                col_copy(h, b, seg, peer, q).start()

    def wait_vec_sends(h, b):
        def each(seg, carry):
            for q in range(CHUNKS):
                @pl.when((c < 3) & (seg <= c))
                def _():
                    row_copy(h, b, seg, 0, q).wait_send()

                @pl.when((c > 0) & (seg >= c))
                def _():
                    row_copy(h, b, seg, 1, q).wait_send()

                for peer in range(3):
                    @pl.when(is_diag & ((col_peers[peer] > c) | (seg >= 2)))
                    def _():
                        col_copy(h, b, seg, peer, q).wait_send()
            return carry

        lax.fori_loop(0, SIDE, each, 0)

    def wait_acc_sends(h):
        def each(seg, carry):
            for q in range(CHUNKS):
                @pl.when(sends(seg))
                def _():
                    red_copy(h, seg, q).wait_send()

                @pl.when(~is_diag & (lower | (seg >= 2)))
                def _():
                    sum_copy(h, seg, 0, diag_dev, q).wait_send()
            return carry

        lax.fori_loop(0, SIDE, each, 0)

    def wait_colvec(h, b, seg):
        for q in range(CHUNKS):
            col_copy(h, b, seg, 0, q).wait_recv()

    def send_sum(h, seg):
        for q in range(CHUNKS):
            @pl.when(same_chip)
            def _():
                sum_copy(h, seg, 0, diag_dev, q).start()

            @pl.when(~same_chip & (seg % 2 != core))
            def _():
                sum_copy(h, seg, 0, (kpt, c, partner), q).start()

    def combine_sums(h):
        def each(i, carry):
            seg = 2 * (1 - i) + core
            for q in range(CHUNKS):
                sum_copy(h, seg, 0, diag_dev, q).wait_recv()
                acc[h, SIDE + seg, rows_of(q)] += col[h, 0, seg, rows_of(q)]
                sum_copy(h, seg, 1, diag_dev, q).start()
            return carry

        @pl.when(~same_chip)
        def _():
            lax.fori_loop(0, jnp.where(lower, 2, 1), each, 0)

    def column_total(h, start, stop):
        def each(i, carry):
            seg = seg_order(i)
            near = (partner > c) | (seg >= 2)
            far = (far0 > c) | (seg >= 2)
            for q in range(CHUNKS):
                @pl.when(near)
                def _():
                    sum_copy(h, seg, 0, diag_dev, q).wait_recv()
                    acc[h, seg, rows_of(q)] += col[h, 0, seg, rows_of(q)]

                @pl.when(far)
                def _():
                    sum_copy(h, seg, 1, diag_dev, q).wait_recv()
                    acc[h, seg, rows_of(q)] += col[h, 1, seg, rows_of(q)]
                start_sum(h, seg, q)
            return carry

        lax.fori_loop(start, stop, each, 0)

    def arrived(h, seg, slot, q):
        pltpu.make_async_remote_copy(
            src_ref=acc.at[h, seg, rows_of(q)], dst_ref=red.at[h, slot, rows_of(q)],
            send_sem=acc_send.at[h, seg, q], recv_sem=red_recv.at[h, slot, q],
            device_id=diag_dev, device_id_type=MESH).wait_recv()
        acc[h, seg, rows_of(q)] += red[h, slot, rows_of(q)]

    def relay(h, seg):
        @pl.when(sends(seg) & incoming(seg))
        def _():
            for q in range(CHUNKS):
                arrived(h, seg, seg, q)
                red_copy(h, seg, q).start()

    def start_sum(h, seg, q):
        @pl.when(sends(seg) & ~incoming(seg))
        def _():
            red_copy(h, seg, q).start()

    def product(left, right, dims):
        return lax.dot_general(left, right, dims, preferred_element_type=jnp.float32)

    first_half = jnp.where(c == 0, 0, 1)

    def slab_load(half, seg):
        rows = pl.ds(pl.multiple_of(half * seg_rows, seg_rows), seg_rows)
        return pltpu.make_async_copy(
            slab_hbm.at[rows, pl.ds(pl.multiple_of(seg * seg_rows, seg_rows), seg_rows)],
            mat.at[seg, rows], mat_sem.at[half, seg])

    def strip_load(seg):
        return pltpu.make_async_copy(
            strip_hbm.at[:, pl.ds(pl.multiple_of(seg * seg_rows, seg_rows), seg_rows)],
            mat.at[seg, pl.ds(2 * seg_rows, seg_rows)], mat_sem.at[2, seg])

    def strip_terms(k, b, seg, first):
        @pl.when(k == 1)
        def _():
            strip_load(seg).wait()
        term = product(vec[b, 0, seg], mat[seg, 2 * seg_rows:], NT)
        strip_acc[...] = jnp.where(first, 0.0, strip_acc[...]) + term

    def take_piece(k, h, b, seg):
        @pl.when(upper)
        def _():
            @pl.when((k == 0) & ((c < 3) | (seg > 0)))
            def _():
                for half in range(2):
                    slab_load(half, seg).wait()
            both = product(vec[b, 0, seg, half_of(h)], mat[seg, :2 * seg_rows], NT)
            for i in range(2):
                acc[h, SIDE + 2 + i] += both[:, i * seg_rows:(i + 1) * seg_rows]

        @pl.when(lower & (seg < 2))
        def _():
            @pl.when(k == 0)
            def _():
                for j in range(SIDE):
                    slab_load(seg, j).wait()

                @pl.when(seg == first_half)
                def _():
                    for j in range(SIDE):
                        slab_load(1 - first_half, j).start()
            rows = pl.ds(pl.multiple_of(seg * seg_rows, seg_rows), seg_rows)
            for j in range(SIDE):
                acc[h, SIDE + j] += product(vec[b, 0, seg, half_of(h)], mat[j, rows], NN)

    def upper_row_terms(h, b, early):
        def each(i, carry):
            seg = seg_order(i)
            acc[h, seg] = (product(vec[b, 1, 2, half_of(h)], mat[seg, :seg_rows], NN)
                           + product(vec[b, 1, 3, half_of(h)], mat[seg, seg_rows:2 * seg_rows], NN))

            @pl.when(i < early)
            def _():
                for q in range(CHUNKS):
                    start_sum(h, seg, q)
            return carry

        lax.fori_loop(0, SIDE, each, 0)

    def lower_row_terms(h, b):
        def each(i, carry):
            seg = (i + c) % SIDE

            @pl.when(i > 0)
            def _():
                wait_colvec(h, b, seg)
            both = product(vec[b, 1, seg, half_of(h)], mat[seg, :2 * seg_rows], NT)
            for half in range(2):
                acc[h, half] += both[:, half * seg_rows:(half + 1) * seg_rows]
            return carry

        lax.fori_loop(0, SIDE, each, 0)

    def finish(k, h, b, next_b):
        wait_vec_sends(h, b)

        for q in range(CHUNKS):
            @pl.when(from_left(c))
            def _():
                arrived(h, c, c, q)

            @pl.when(from_right(c))
            def _():
                arrived(h, c, SIDE, q)

        center = jnp.where(h == 0, CEN_OCC, CEN_VIRT)
        applied = acc[h, c] + strip_acc[half_of(h)]
        scaled = (applied - center * cur[h]) * (1.0 / HALF_WIDTH)
        first = k < HALVES
        nxt = jnp.where(first, scaled, 2.0 * scaled - prev[h])
        prev[h] = cur[h]
        cur[h] = nxt

        @pl.when(k + HALVES < UNITS)
        def _():
            vec[next_b, 0, c, half_of(h)] = nxt.astype(jnp.bfloat16)
            for q in range(CHUNKS):
                send_row(h, next_b, c, True, True, q)
                send_col(h, next_b, c, q)

    barrier = pltpu.get_barrier_semaphore()

    @pl.when(c > 0)
    def _():
        pl.semaphore_signal(barrier, inc=1, device_id=(kpt, c - 1, r), device_id_type=MESH)

    @pl.when(c < 3)
    def _():
        pl.semaphore_signal(barrier, inc=1, device_id=(kpt, c + 1, r), device_id_type=MESH)

    for peer in range(3):
        pl.semaphore_signal(barrier, inc=1, device_id=(kpt, c, col_peers[peer]), device_id_type=MESH)

    def load_block(i, carry):
        seg = (c + i) % SIDE

        @pl.when(upper)
        def _():
            for half in range(2):
                slab_load(half, seg).start()

        @pl.when(lower)
        def _():
            slab_load(first_half, seg).start()
        return carry

    lax.fori_loop(0, SIDE, load_block, 0)
    for h, src in enumerate((occ_ref, virt_ref)):
        cur[h] = src[...]
        prev[h] = jnp.zeros_like(src)
        vec[0, 0, c, half_of(h)] = src[...].astype(jnp.bfloat16)
    pl.semaphore_wait(barrier, 3 + (c > 0).astype(jnp.int32) + (c < 3).astype(jnp.int32))
    for q in range(CHUNKS):
        send_row(0, 0, c, True, True, q)
        send_col(0, 0, c, q)

    def slot(k, carry):
        h = k % 2
        b = (k // 2) % 2
        last = k - 1
        lh = (k + 1) % 2
        lb = ((k + 1) // 2 + 1) % 2
        live = k < UNITS
        older = k >= 1
        final = k == UNITS - 1
        early = jnp.where(final, SIDE, EARLY)

        @pl.when(live)
        def _():
            @pl.when(k >= HALVES)
            def _():
                wait_acc_sends(h)

            def clear(i, cc):
                acc[h, i] = jnp.zeros(acc.shape[2:], acc.dtype)
                return cc

            lax.fori_loop(0, 2 * SIDE, clear, 0)

        def arrivals(d, cc):
            for s in (1, 0):
                for q in range(CHUNKS):
                    seg = c + (2 * s - 1) * d

                    @pl.when(live & (seg >= 0) & (seg < SIDE) & (d > 0))
                    def _():
                        row_copy(h, b, seg, 0, q).wait_recv()
                        send_row(h, b, seg, s == 1, s == 0, q)
                        send_col(h, b, seg, q)

            @pl.when(older & is_diag & (c >= 2) & (d == 1))
            def _():
                column_total(lh, 0, SIDE)

            def hop(i):
                @pl.when(older & (c > 0) & (c < 3) & (i >= 0) & (i < 3))
                def _():
                    relay(lh, jnp.where(c == 1, jnp.where(i == 2, 0, 3 - i), jnp.where(i == 2, 3, i)))

            hop(d - 1 - 5 * (d == 3))

            @pl.when((k == 0) & (d == 2))
            def _():
                for q in range(CHUNKS):
                    send_row(1, 0, c, True, True, q)
                    send_col(1, 0, c, q)

            def use(s, ccc):
                seg = c + (2 * s - 1) * d

                @pl.when(live & (seg >= 0) & (seg < SIDE) & ((d > 0) | (s == 0)))
                def _():
                    take_piece(k, h, b, seg)

                    @pl.when(h == 1)
                    def _():
                        strip_terms(k, b, seg, d == 0)
                return ccc

            lax.fori_loop(0, 2, use, 0)

            hop(jnp.where(d == 2, 2, -1))

            @pl.when(live & lower & (d == jnp.where(c == 2, 2, 1)))
            def _():
                wait_colvec(h, b, c)

                def each(i, ccc):
                    send_sum(h, seg_order(i))
                    return ccc

                lax.fori_loop(0, SIDE, each, 0)

            @pl.when(live & lower & (d == 2))
            def _():
                combine_sums(h)

            @pl.when(live & upper & (d == 2))
            def _():
                wait_colvec(h, b, 2)
                wait_colvec(h, b, 3)

                @pl.when((k == 0) & (c == 3))
                def _():
                    for half in range(2):
                        slab_load(half, 0).wait()
                upper_row_terms(h, b, early)
            return cc

        lax.fori_loop(0, SIDE, arrivals, 0)

        @pl.when(k == 0)
        def _():
            for j in range(SIDE):
                strip_load(j).start()

        @pl.when(live & upper)
        def _():
            send_sum(h, 2)
            send_sum(h, 3)

        @pl.when(live & lower)
        def _():
            lower_row_terms(h, b)

        @pl.when(live & is_diag & (c == 0))
        def _():
            column_total(h, 0, 2)

        def send_terms():
            @pl.when(live & ~is_diag)
            def _():
                def each(i, cc):
                    for q in range(CHUNKS):
                        start_sum(h, seg_order(i), q)
                    return cc

                lax.fori_loop(jnp.where(upper, early, 0), SIDE, each, 0)

            @pl.when(live & upper)
            def _():
                combine_sums(h)

            @pl.when(live & is_diag & (c < 2))
            def _():
                column_total(h, jnp.where(c == 0, 2, 0), SIDE)

        @pl.when(final)
        def _():
            send_terms()

        @pl.when(older)
        def _():
            finish(last, lh, lb, 1 - lb)

        @pl.when(~final)
        def _():
            send_terms()
        return carry

    lax.fori_loop(0, UNITS + 1, slot, 0)
    for h in range(HALVES):
        wait_acc_sends(h)
    for h in range(HALVES):
        out[h * n_vecs:(h + 1) * n_vecs] = cur[h]


def solution(mesh):
    slab_spec = P(("kpt", "row"), "col", None, None)
    diag_spec = P(("kpt", "row"), "col", None)
    vec_spec = P(("kpt", "row", "col"), None)

    def local_filter(h_slab, h_diag, vec_occ, vec_virt):
        seg_rows, n_vecs = vec_occ.shape
        panel = (n_vecs, seg_rows)
        vmem = pl.BlockSpec(memory_space=pltpu.VMEM)
        hbm = pl.BlockSpec(memory_space=pl.ANY)
        dma = pltpu.SemaphoreType.DMA
        both = pl.pallas_call(
            filter_kernel,
            out_shape=jax.ShapeDtypeStruct((HALVES * n_vecs, seg_rows), jnp.float32),
            in_specs=[hbm, hbm, vmem, vmem],
            out_specs=vmem,
            scratch_shapes=[
                pltpu.VMEM((SIDE, 3 * seg_rows, seg_rows), jnp.bfloat16),
                pltpu.VMEM((2, 2, SIDE, HALVES * n_vecs, seg_rows), jnp.bfloat16),
                pltpu.VMEM((HALVES, 2 * SIDE) + panel, jnp.float32),
                pltpu.VMEM((HALVES * n_vecs, seg_rows), jnp.float32),
                pltpu.VMEM((HALVES, SIDE + 1) + panel, jnp.float32),
                pltpu.VMEM((HALVES, 2, SIDE) + panel, jnp.float32),
                pltpu.VMEM((HALVES,) + panel, jnp.float32),
                pltpu.VMEM((HALVES,) + panel, jnp.float32),
                dma((3, SIDE)),
                dma((HALVES, 5, SIDE, CHUNKS)),
                dma((HALVES, 2, SIDE, CHUNKS)),
                dma((HALVES, 2, SIDE, CHUNKS)),
                dma((HALVES, 2 * SIDE, CHUNKS)),
                dma((HALVES, SIDE + 1, CHUNKS)),
                dma((HALVES, 2, SIDE, CHUNKS)),
            ],
            compiler_params=pltpu.CompilerParams(
                collective_id=0, has_side_effects=True, vmem_limit_bytes=67_000_000),
        )(h_slab[0, 0], h_diag[0], vec_occ.T, vec_virt.T)
        return both[:n_vecs].T, both[n_vecs:].T

    return jax.shard_map(local_filter, mesh=mesh, in_specs=(slab_spec, diag_spec, vec_spec, vec_spec), out_specs=(vec_spec, vec_spec), check_vma=False)
```
